32 devices in a mesh: grp: 2 (over y), band: 4 (over z), mem: 2 (over x), fld: 2 (over core).
Axes of the slice: x: 2, y: 2, z: 4, core: 2. Of those that a mesh axis runs over, the one named last changes fastest.
Arguments:
- surface_fields: bfloat16 [16, 8, 8, 65536], P(('grp', 'mem'), 'fld', None, 'band'), parts along dimension 0, may hold values from -8 to 8
- land_mask: int32 [65536], P('band'), may hold values from 0 to 1, as said below
- source_area: float32 [65536], P('band'), may hold values from 0.5 to 1.5
- target_area: float32 [16384], P('band'), may hold values from 0.75 to 1.25
- weight_tiles: bfloat16 [16, 128, 128], replicated, may hold values from -1 to 1
- tile_of: int32 [128, 24], P('band'), may hold values from 0 to 15
- block_of: int32 [128, 24], P('band'), may hold values from 0 to 191, as said below
- live_slots: int32 [128], P('band'), may hold values from 1 to 24, as said below
Outputs:
- regridded: float32 [16, 8, 8, 16384], P(('grp', 'mem'), 'fld', None, 'band'), parts along dimension 0
- conserved: float32 [16, 8, 8], P(('grp', 'mem'), 'fld'), parts along dimension 0
- ensemble: float32 [16, 8], P(('grp', 'fld')), parts along dimension 0
The draws below stay inside these ranges and needn't reach their ends.
There are 2 independent parts, one for each index of `grp`. The reference program is written for one: setup_inputs(seed, part) draws one part's arguments, and reference() takes and returns one part's arrays. A program takes and returns all parts, laid end to end along the dimension named above; an argument that names none is the same for every part. Nothing has to cross between parts.
Inputs may be any that keep to these rules, and one draw needn't show every extreme that they name: `land_mask`: 1 marks ocean, 0 land. `block_of`: for the target block at place j (0 to 31) within its band, every entry lies in 4 * j to 4 * j + 4 + 2 * 32 - 1; values under 32 name the lower band's last blocks, values from 160 on the higher band's first blocks. `live_slots`: slots from this count on are unused.
All inputs are finite; a program needn't handle non-finite values.
Results may differ from the reference program's by a relative error of at most 0.0014.
Values may be sent and summed in bfloat16 or wider, within the bound.
No kernel may reach another device: no remote copies, remote signals or barrier semaphores. Data moves between devices by JAX's collectives and lax.ppermute only.
A program may use at most 64 MiB of HBM per device.

```python
import jax
import jax.numpy as jnp
from jax import lax

MEMBERS = 8
FIELDS = 8
SNAPSHOTS = 8
TILE_CELLS = 128
TGT_BLK_DEV = 32
STRIDE = 4
HALO_BLK = 32
SLOT_COUNT = 24
TILE_COUNT = 16
SRC_BLK_DEV = 128
SRC_BLOCKS = 512
TGT_BLOCKS = 128
SRC_CELLS = 65536
TGT_CELLS = 16384


def draw_surface_fields(key, part):
    first_key, second_key, third_key = jax.random.split(key, 3)
    shape = (MEMBERS, FIELDS, SNAPSHOTS, SRC_BLOCKS, TILE_CELLS)
    offset = jax.random.uniform(first_key, (MEMBERS, FIELDS, SNAPSHOTS, 1, 1), jnp.float32, -1.0, 1.0)
    noise = jnp.clip(jax.random.normal(third_key, shape, jnp.float32), -5.0, 5.0)
    regional = 0.5 * jnp.clip(jax.random.normal(second_key, (MEMBERS, FIELDS, SNAPSHOTS, SRC_BLOCKS, 1), jnp.float32), -2.0, 2.0)
    values = offset + regional + noise
    return values.reshape(MEMBERS, FIELDS, SNAPSHOTS, SRC_CELLS).astype(jnp.bfloat16)


def draw_land_mask(key, part):
    first_key, second_key, third_key = jax.random.split(key, 3)
    band_count = SRC_CELLS // (SRC_BLK_DEV * TILE_CELLS)
    band_level = jax.random.randint(first_key, (band_count, 1, 1), 25, 101)
    region_level = jax.random.randint(second_key, (band_count, SRC_BLK_DEV, 1), 40, 101)
    cell_draw = jax.random.randint(third_key, (band_count, SRC_BLK_DEV, TILE_CELLS), 0, 10000)
    ocean = (cell_draw < band_level * region_level).astype(jnp.int32)
    return ocean.reshape(SRC_CELLS)


def draw_weight_tiles(key, part):
    fan = SLOT_COUNT * TILE_CELLS
    shape = (TILE_COUNT, TILE_CELLS, TILE_CELLS)
    noise = jnp.clip(jax.random.normal(key, shape, jnp.float32), -5.0, 5.0)
    mean_part = 1.0
    return ((mean_part + noise * jnp.sqrt(jnp.float32(fan))) / fan).astype(jnp.bfloat16)


def draw_block_of(key, part):
    position = jnp.arange(TGT_BLOCKS, dtype=jnp.int32) % TGT_BLK_DEV
    offsets = jax.random.randint(key, (TGT_BLOCKS, SLOT_COUNT), 0, STRIDE + 2 * HALO_BLK)
    picks = STRIDE * position[:, None] + offsets
    picks = picks.at[0, 0].set(0)
    picks = picks.at[TGT_BLOCKS - 1, 0].set(STRIDE * TGT_BLK_DEV + 2 * HALO_BLK - 1)
    return picks.astype(jnp.int32)


def draw_live_slots(key, part):
    first_key, second_key = jax.random.split(key, 2)
    band_count = TGT_BLOCKS // TGT_BLK_DEV
    tops = jax.random.randint(first_key, (band_count,), SLOT_COUNT // 4 + 1, SLOT_COUNT + 1)
    band_top = jnp.repeat(tops, TGT_BLK_DEV)
    counts = jax.random.randint(second_key, (TGT_BLOCKS,), 1, band_top + 1)
    return counts.at[0].set(SLOT_COUNT).astype(jnp.int32)


def set_ends(array, stream_key, least, largest):
    longest = array.shape.index(max(array.shape))
    spots = []
    for shift in (0, 1):
        where = [jax.random.randint(jax.random.fold_in(stream_key, axis), (), 0, length) for axis, length in enumerate(array.shape)]
        where[longest] = (where[longest] + shift) % array.shape[longest]
        spots.append(tuple(where))
    return array.at[spots[0]].set(least).at[spots[1]].set(largest)


def level_of(key, extent, pieces, least, high):
    factor_of, own = 1.0, jax.random.fold_in(key, 6)
    for dim, blocks in pieces:
        draws = jnp.exp(jax.random.uniform(jax.random.fold_in(own, dim), (blocks,), jnp.float32, least / len(pieces), high / len(pieces)))
        factor_of = factor_of * jnp.repeat(draws, extent[dim] // blocks).reshape([-1 if axis == dim else 1 for axis in range(len(extent))])
    return factor_of


def setup_inputs(seed: int = 0, part: int = 0) -> dict:
    splits = jax.random.split(jax.random.key(seed), 9)
    own_keys = jax.random.split(jax.random.fold_in(splits[8], part), 9)
    return {
        "surface_fields": draw_surface_fields(jax.random.fold_in(jax.random.fold_in(splits[8], part), 71), part),
        "land_mask": draw_land_mask(jax.random.fold_in(splits[8], 71), part),
        "source_area": jnp.clip(0.5 + 1.0 * jax.random.uniform(splits[2], (SRC_CELLS,), jnp.float32) ** level_of(splits[2], (SRC_CELLS,), ((0, 4),), -0.2, 0.2), 0.5, 1.5),
        "target_area": jnp.clip(0.75 + 0.5 * jax.random.uniform(splits[3], (TGT_CELLS,), jnp.float32) ** level_of(splits[3], (TGT_CELLS,), ((0, 4),), -0.2, 0.2), 0.75, 1.25),
        "weight_tiles": draw_weight_tiles(jax.random.fold_in(splits[8], 71), part),
        "tile_of": set_ends(jax.random.randint(splits[5], (TGT_BLOCKS, SLOT_COUNT), 0, TILE_COUNT), jax.random.fold_in(splits[5], 1), 0, TILE_COUNT - 1).astype(jnp.int32),
        "block_of": draw_block_of(jax.random.fold_in(splits[8], 71), part),
        "live_slots": draw_live_slots(jax.random.fold_in(splits[8], 71), part),
    }


def reference(surface_fields, land_mask, source_area, target_area, weight_tiles, tile_of, block_of, live_slots):
    columns = MEMBERS * FIELDS * SNAPSHOTS
    weighted = (source_area * land_mask.astype(jnp.float32) * surface_fields.astype(jnp.float32)).astype(jnp.bfloat16)
    flat = weighted.reshape(columns, SRC_BLOCKS, TILE_CELLS)
    padding = jnp.zeros((columns, HALO_BLK, TILE_CELLS), jnp.bfloat16)
    padded = jnp.concatenate([padding, flat, padding], axis=1)
    owner = jnp.arange(TGT_BLOCKS, dtype=jnp.int32) // TGT_BLK_DEV
    picks = (owner[:, None] * SRC_BLK_DEV + block_of).astype(jnp.int32)

    def one_slot(running, position):
        chosen = jnp.take(padded, picks[:, position], axis=1).astype(jnp.float32)
        weights = jnp.take(weight_tiles, tile_of[:, position], axis=0).astype(jnp.float32)
        usable = (position < live_slots)[:, None, None]
        weights = jnp.where(usable, weights, jnp.zeros((), jnp.float32))
        running = running + jnp.einsum("cnb,nbd->cnd", chosen, weights, precision=lax.Precision.HIGHEST)
        return running, None

    start = jnp.zeros((columns, TGT_BLOCKS, TILE_CELLS), jnp.float32)
    raw_sums, unused = lax.scan(one_slot, start, jnp.arange(SLOT_COUNT, dtype=jnp.int32))
    raw_sums = raw_sums.reshape(columns, TGT_CELLS)
    source_total = jnp.sum(weighted.reshape(columns, SRC_CELLS).astype(jnp.float32), axis=1)
    target_total = jnp.sum(raw_sums, axis=1)
    area_total = jnp.sum(target_area)
    regridded = raw_sums / target_area[None, :] + ((source_total - target_total) / area_total)[:, None]
    conserved = (source_total / area_total).reshape(MEMBERS, FIELDS, SNAPSHOTS)
    ensemble = jnp.sum(conserved, axis=0) / MEMBERS
    return regridded.reshape(MEMBERS, FIELDS, SNAPSHOTS, TGT_CELLS), conserved, ensemble
```

```python
import functools

import jax
import jax.numpy as jnp
from jax import lax
from jax.experimental import pallas as pl
from jax.experimental.pallas import tpu as pltpu
from jax.sharding import PartitionSpec as P


MEMBERS = 8
HALO_BLK = 32
CHUNK = 4
UNROLL = 4
PIECES = 8
PLACE_BITS = 16

VMEM = pl.BlockSpec(memory_space=pltpu.VMEM)
SMEM = pl.BlockSpec(memory_space=pltpu.SMEM)
ANY = pl.BlockSpec(memory_space=pl.ANY)


def params(mib):
    return pltpu.CompilerParams(vmem_limit_bytes=mib * 1024 * 1024)


def row_of(acc):
    return jnp.sum(acc.T, axis=0, keepdims=True)


def list_items(tile_of, block_of, live, columns, bounds, shift, blank, at, out):
    slots = tile_of.shape[0]
    last = out.shape[1] - 1

    def one_target(n, items):
        column = columns + n

        def one_slot(k, place):
            block = block_of[k, column] - HALO_BLK
            out[0, place] = (tile_of[k, column] << PLACE_BITS) + block + shift
            inside = jnp.logical_and(block >= bounds[0], block < bounds[1])
            return place + jnp.where(inside, 1, 0)

        place = lax.fori_loop(0, live[column], one_slot, items * CHUNK)
        for q in range(CHUNK):
            out[0, place + q] = blank
        for q in range(-(-slots // CHUNK)):
            out[0, at + items + q] = n
        return lax.div(place + CHUNK - 1, CHUNK)

    def listed(count):
        items = lax.fori_loop(0, count, one_target, 0)
        for q in range(UNROLL * CHUNK):
            out[0, items * CHUNK + q] = blank
        for q in range(UNROLL):
            out[0, at + items + q] = 0
        out[0, last] = items

    return listed


def list_sizes(targets, slots):
    items = targets * -(-slots // CHUNK) + UNROLL
    at = items * CHUNK
    return at, -(-(at + items + 8) // 128) * 128


def edge_body(own_blocks, blank, edge, tile_of, block_of, live, low, high):
    slots, tgt_count = tile_of.shape
    at, _ = list_sizes(edge, slots)
    list_items(
        tile_of, block_of, live, 0, (-HALO_BLK, 0), own_blocks, blank, at, low
    )(edge)
    list_items(
        tile_of, block_of, live, tgt_count - edge, (own_blocks, own_blocks + HALO_BLK),
        -own_blocks, blank, at, high,
    )(edge)


def weigh_body(
    fields_hbm, mask_ref, area_ref, target_ref, tiles_hbm, tile_of, block_of, live,
    weighted, tiles, totals, items, staged, sems,
):
    columns, cells = weighted.shape
    tile_count, tile, lanes = tiles_hbm.shape
    own_blocks = cells // tile
    slots, tgt_count = tile_of.shape
    piece = cells // PIECES
    step = 4 * tile
    copies = [
        pltpu.make_async_copy(
            fields_hbm.at[:, pl.ds(n * piece, piece)],
            staged.at[:, pl.ds(n * piece, piece)],
            sems.at[n],
        )
        for n in range(PIECES)
    ]
    for copy in copies:
        copy.start()
    tile_copy = pltpu.make_async_copy(tiles_hbm, tiles.at[pl.ds(0, tile_count)], sems.at[PIECES])
    tile_copy.start()
    tiles[tile_count] = jnp.zeros((tile, lanes), tiles.dtype)
    at, _ = list_sizes(tgt_count, slots)
    list_items(
        tile_of, block_of, live, 0, (0, own_blocks), 0, tile_count << PLACE_BITS, at, items
    )(tgt_count)
    acc = jnp.zeros((columns, tile), jnp.float32)
    for n in range(PIECES):
        copies[n].wait()

        def one(k, acc):
            at = pl.ds(pl.multiple_of(n * piece + k * step, step), step)
            factor = area_ref[:, at] * mask_ref[:, at].astype(jnp.float32)
            value = (factor * staged[:, at].astype(jnp.float32)).astype(jnp.bfloat16)
            weighted[:, at] = value
            wide = value.astype(jnp.float32)
            for q in range(4):
                acc = acc + wide[:, q * tile : (q + 1) * tile]
            return acc

        acc = lax.fori_loop(0, piece // step, one, acc)
    own = row_of(acc)
    area = jnp.sum(target_ref[...], axis=1, keepdims=True)
    rows = lax.broadcasted_iota(jnp.int32, (8, columns), 0)
    totals[...] = jnp.where(rows == 0, own, jnp.where(rows == 1, area, 0.0))
    tile_copy.wait()


def run_items(items, at, weighted, tiles, out):
    tile = tiles.shape[1]
    count = items[0, items.shape[1] - 1]
    out[...] = jnp.zeros(out.shape, out.dtype)

    def one(step, nothing):
        base = step * UNROLL
        products = []
        for u in range(UNROLL):
            left, right = [], []
            for q in range(CHUNK):
                code = items[0, (base + u) * CHUNK + q]
                block = code & ((1 << PLACE_BITS) - 1)
                left.append(weighted[:, pl.ds(pl.multiple_of(block * tile, tile), tile)])
                right.append(tiles[code >> PLACE_BITS])
            products.append(
                jnp.dot(
                    jnp.concatenate(left, axis=1),
                    jnp.concatenate(right, axis=0),
                    preferred_element_type=jnp.float32,
                )
            )
        for u in range(UNROLL):
            target = items[0, at + base + u]
            place = pl.ds(pl.multiple_of(target * tile, tile), tile)
            out[:, place] = out[:, place] + products[u]
        return nothing

    lax.fori_loop(0, lax.div(count + UNROLL - 1, UNROLL), one, 0)
    acc = out[:, :tile]
    for n in range(1, out.shape[1] // tile):
        acc = acc + out[:, n * tile : (n + 1) * tile]
    return acc


def reach_body(at, up_items, down_items, weighted, tiles, to_up, to_down, sums, first, second):
    acc = run_items(up_items, at, weighted, tiles, first)
    to_up[...] = first[...].astype(to_up.dtype)
    acc = acc + run_items(down_items, at, weighted, tiles, second)
    to_down[...] = second[...].astype(to_down.dtype)
    sums[...] = jnp.broadcast_to(row_of(acc), sums.shape)


def local_body(at, items, weighted, tiles, reach_sums, raw, sums):
    acc = run_items(items, at, weighted, tiles, raw)
    sums[...] = reach_sums[...] + row_of(acc)


def finish_body(raw, from_down, from_up, target, totals, sums, out_hbm, staged, sems):
    columns, cells = raw.shape
    edge = from_down.shape[1]
    piece = edge // 2
    pieces = cells // piece
    correction = (totals[0:1] - sums[0:1]) / totals[1:2]
    spread = jnp.broadcast_to(correction, (128, columns)).T
    spread = jnp.concatenate([spread] * (piece // 128), axis=1)
    copies = []
    for n in range(pieces):
        at = pl.ds(n * piece, piece)
        value = raw[:, at]
        if n * piece < edge:
            value = value + from_down[:, at].astype(jnp.float32)
        if (n + 1) * piece > cells - edge:
            begin = n * piece - (cells - edge)
            value = value + from_up[:, pl.ds(begin, piece)].astype(jnp.float32)
        staged[:, at] = value / target[:, at] + spread
        copies.append(pltpu.make_async_copy(staged.at[:, at], out_hbm.at[:, at], sems.at[n]))
        copies[n].start()
    for copy in copies:
        copy.wait()


def total_over(values, axis):
    size = lax.axis_size(axis)
    if size & (size - 1) or size > 8:
        return lax.psum(values, axis)
    terms = [values]
    for step in range(1, size):
        terms.append(lax.ppermute(values, axis, [(i, i ^ step) for i in range(size)]))
    while len(terms) > 1:
        terms = [a + b for a, b in zip(terms[0::2], terms[1::2])]
    return terms[0]


def regrid(
    surface_fields, land_mask, source_area, target_area, weight_tiles, tile_of, block_of, live_slots
):
    members, fields, snapshots, cells = surface_fields.shape
    columns = members * fields * snapshots
    tile_count, tile, _ = weight_tiles.shape
    tgt_count, slots = tile_of.shape
    own_blocks = cells // tile
    stride = own_blocks // tgt_count
    edge = -(-HALO_BLK // stride)
    size = lax.axis_size("band")
    up = [(i, i + 1) for i in range(size - 1)]
    down = [(i + 1, i) for i in range(size - 1)]
    f32 = jnp.float32

    blank = tile_count << PLACE_BITS
    at_edge, edge_size = list_sizes(edge, slots)
    at_own, own_size = list_sizes(tgt_count, slots)
    tables = (tile_of.T, block_of.T, live_slots)
    low, high = pl.pallas_call(
        functools.partial(edge_body, own_blocks, blank, edge),
        out_shape=(jax.ShapeDtypeStruct((1, edge_size), jnp.int32),) * 2,
        in_specs=[SMEM] * 3,
        out_specs=(SMEM, SMEM),
        compiler_params=params(8),
        name="edges",
    )(*tables)
    up_list = lax.ppermute(low, "band", down)
    down_list = lax.ppermute(high, "band", up)

    weighted, tiles, totals, items = pl.pallas_call(
        weigh_body,
        out_shape=(
            jax.ShapeDtypeStruct((columns, cells), jnp.bfloat16),
            jax.ShapeDtypeStruct((tile_count + 1, tile, tile), jnp.bfloat16),
            jax.ShapeDtypeStruct((8, columns), f32),
            jax.ShapeDtypeStruct((1, own_size), jnp.int32),
        ),
        in_specs=[ANY, VMEM, VMEM, VMEM, ANY, SMEM, SMEM, SMEM],
        out_specs=(VMEM, VMEM, VMEM, SMEM),
        scratch_shapes=[
            pltpu.VMEM((columns, cells), jnp.bfloat16),
            pltpu.SemaphoreType.DMA((PIECES + 1,)),
        ],
        compiler_params=params(16),
        name="weigh",
    )(
        pltpu.with_memory_space_constraint(surface_fields.reshape(columns, cells), pltpu.HBM),
        land_mask.reshape(1, cells),
        source_area.reshape(1, cells),
        target_area.reshape(1, tgt_count * tile),
        pltpu.with_memory_space_constraint(weight_tiles, pltpu.HBM),
        *tables,
    )
    totals = total_over(totals, "band")

    to_up, to_down, reach_sums = pl.pallas_call(
        functools.partial(reach_body, at_edge),
        out_shape=(
            jax.ShapeDtypeStruct((columns, edge * tile), jnp.bfloat16),
            jax.ShapeDtypeStruct((columns, edge * tile), jnp.bfloat16),
            jax.ShapeDtypeStruct((8, columns), f32),
        ),
        in_specs=[SMEM, SMEM, VMEM, VMEM],
        out_specs=(VMEM, VMEM, VMEM),
        scratch_shapes=[pltpu.VMEM((columns, edge * tile), f32)] * 2,
        compiler_params=params(8),
        name="reach",
    )(up_list, down_list, weighted, tiles)
    from_down = lax.ppermute(to_up, "band", up)
    from_up = lax.ppermute(to_down, "band", down)

    raw, sums = pl.pallas_call(
        functools.partial(local_body, at_own),
        out_shape=(
            jax.ShapeDtypeStruct((columns, tgt_count * tile), f32),
            jax.ShapeDtypeStruct((8, columns), f32),
        ),
        in_specs=[SMEM, VMEM, VMEM, VMEM],
        out_specs=(VMEM, VMEM),
        compiler_params=params(8),
        name="local",
    )(items, weighted, tiles, reach_sums)
    sums = total_over(sums, "band")

    piece_count = 2 * tgt_count // edge
    regridded = pl.pallas_call(
        finish_body,
        out_shape=jax.ShapeDtypeStruct((columns, tgt_count * tile), f32),
        in_specs=[VMEM] * 6,
        out_specs=ANY,
        scratch_shapes=[
            pltpu.VMEM((columns, tgt_count * tile), f32),
            pltpu.SemaphoreType.DMA((piece_count,)),
        ],
        compiler_params=params(16),
        name="finish",
    )(raw, from_down, from_up, target_area.reshape(1, tgt_count * tile), totals, sums)

    conserved = (totals[0] / totals[1]).reshape(members, fields, snapshots)
    ensemble = total_over(jnp.sum(conserved, axis=0), "mem") / MEMBERS
    return regridded.reshape(members, fields, snapshots, tgt_count * tile), conserved, ensemble


def solution(mesh):
    placed = (
        P(("grp", "mem"), "fld", None, "band"),
        P("band"),
        P("band"),
        P("band"),
        P(),
        P("band", None),
        P("band", None),
        P("band"),
    )
    return jax.shard_map(
        regrid,
        mesh=mesh,
        in_specs=placed,
        out_specs=(
            P(("grp", "mem"), "fld", None, "band"),
            P(("grp", "mem"), "fld", None),
            P(("grp", "fld"), None),
        ),
        check_vma=False,
    )
```

```python
import functools

import jax
import jax.numpy as jnp
from jax import lax
from jax.experimental import pallas as pl
from jax.experimental.pallas import tpu as pltpu
from jax.sharding import PartitionSpec as P


MEMBERS = 8
HALO_BLK = 32
CHUNK = 4
CHUNK_BITS = 2
UNROLL = 4
UNROLL_BITS = 2
PIECES = 8
PLACE_BITS = 16

VMEM = pl.BlockSpec(memory_space=pltpu.VMEM)
SMEM = pl.BlockSpec(memory_space=pltpu.SMEM)
ANY = pl.BlockSpec(memory_space=pl.ANY)


def params(mib):
    return pltpu.CompilerParams(vmem_limit_bytes=mib * 1024 * 1024)


def row_of(acc):
    return jnp.sum(acc.T, axis=0, keepdims=True)


def packed(mask, code, blank):
    slots, targets = code.shape
    ones = jnp.where(mask, 1.0, 0.0)
    above = lax.broadcasted_iota(jnp.int32, (slots, slots), 0)
    below = lax.broadcasted_iota(jnp.int32, (slots, slots), 1)
    before = jnp.where(below < above, 1.0, 0.0).astype(jnp.bfloat16)
    rank = jnp.dot(before, ones.astype(jnp.bfloat16), preferred_element_type=jnp.float32)
    rank = jnp.where(mask, rank, -1.0).astype(jnp.int32)
    extra = (code - blank).astype(jnp.float32)
    rows = [
        jnp.sum(jnp.where(rank == p, extra, 0.0), axis=0, keepdims=True) for p in range(slots)
    ]
    body = jnp.concatenate(rows, axis=0).astype(jnp.int32) + blank
    counts = jnp.sum(ones, axis=0, keepdims=True).astype(jnp.int32)
    row = lax.broadcasted_iota(jnp.int32, (8, targets), 0)
    return jnp.concatenate([body, jnp.where(row == 0, counts, blank)], axis=0)


def edge_body(own_blocks, blank, tile_hbm, block_hbm, live_hbm, own, low, high, tiles, blocks, live, sems):
    copies = [
        pltpu.make_async_copy(source, place, sems.at[n])
        for n, (source, place) in enumerate(((tile_hbm, tiles), (block_hbm, blocks), (live_hbm, live)))
    ]
    for copy in copies:
        copy.start()
    for copy in copies:
        copy.wait()
    band = lax.axis_index("band")
    slot = lax.broadcasted_iota(jnp.int32, tiles.shape, 0)
    alive = slot < live[...]
    block = blocks[...] - HALO_BLK
    code = (tiles[...] << PLACE_BITS) + block
    below = jnp.where(band > 0, 0, -HALO_BLK)
    above = jnp.where(band < lax.axis_size("band") - 1, own_blocks, own_blocks + HALO_BLK)
    low[...] = packed(alive & (block < below), code + own_blocks, blank)
    high[...] = packed(alive & (block >= above), code - own_blocks, blank)
    own[...] = packed(alive & (block >= 0) & (block < own_blocks), code, blank)


def weigh_body(
    fields_hbm, mask_hbm, area_hbm, target_hbm, tiles_hbm,
    weighted, totals, tiles, fields, mask, source, target, sems,
):
    columns, cells = weighted.shape
    tile_count, tile, lanes = tiles_hbm.shape
    step = 4 * tile
    piece = cells // PIECES
    small = [
        pltpu.make_async_copy(mask_hbm, mask, sems.at[PIECES]),
        pltpu.make_async_copy(area_hbm, source, sems.at[PIECES + 1]),
        pltpu.make_async_copy(target_hbm, target, sems.at[PIECES + 2]),
        pltpu.make_async_copy(tiles_hbm, tiles.at[pl.ds(0, tile_count)], sems.at[PIECES + 3]),
    ]
    copies = [
        pltpu.make_async_copy(
            fields_hbm.at[:, pl.ds(n * piece, piece)],
            fields.at[:, pl.ds(n * piece, piece)],
            sems.at[n],
        )
        for n in range(PIECES)
    ]
    for copy in small[:3] + copies + small[3:]:
        copy.start()
    tiles[tile_count] = jnp.zeros((tile, lanes), tiles.dtype)
    for copy in small[:3]:
        copy.wait()
    area = jnp.sum(target[...], axis=1, keepdims=True)
    acc = jnp.zeros((columns, tile), jnp.float32)
    for n in range(PIECES):
        copies[n].wait()

        def one(k, acc):
            at = pl.ds(pl.multiple_of(n * piece + k * step, step), step)
            factor = source[:, at] * mask[:, at].astype(jnp.float32)
            value = (factor * fields[:, at].astype(jnp.float32)).astype(jnp.bfloat16)
            weighted[:, at] = value
            wide = value.astype(jnp.float32)
            for q in range(4):
                acc = acc + wide[:, q * tile : (q + 1) * tile]
            return acc

        acc = lax.fori_loop(0, piece // step, one, acc)
    own = row_of(acc)
    rows = lax.broadcasted_iota(jnp.int32, (8, columns), 0)
    totals[...] = jnp.where(rows == 0, own, jnp.where(rows == 1, area, 0.0))
    small[3].wait()


def run_items(codes, first, weighted, tiles, out, work):
    tile = tiles.shape[1]
    slots = codes.shape[0] - 8
    chunks = slots // CHUNK
    out[...] = jnp.zeros(out.shape, out.dtype)

    def one_target(n, items):
        for q in range(chunks):
            work[items + q] = (q << PLACE_BITS) + n
        return items + ((codes[slots, first + n] + CHUNK - 1) >> CHUNK_BITS)

    count = lax.fori_loop(0, out.shape[1] // tile, one_target, 0)
    for q in range(UNROLL):
        work[count + q] = (slots + 4) // CHUNK << PLACE_BITS

    def one(step, nothing):
        products = []
        for u in range(UNROLL):
            item = work[step * UNROLL + u]
            row = (item >> PLACE_BITS) * CHUNK
            column = first + (item & ((1 << PLACE_BITS) - 1))
            left, right = [], []
            for q in range(CHUNK):
                code = codes[row + q, column]
                block = code & ((1 << PLACE_BITS) - 1)
                left.append(weighted[:, pl.ds(pl.multiple_of(block * tile, tile), tile)])
                right.append(tiles[code >> PLACE_BITS])
            products.append(
                jnp.dot(
                    jnp.concatenate(left, axis=1),
                    jnp.concatenate(right, axis=0),
                    preferred_element_type=jnp.float32,
                )
            )
        for u in range(UNROLL):
            target = work[step * UNROLL + u] & ((1 << PLACE_BITS) - 1)
            place = pl.ds(pl.multiple_of(target * tile, tile), tile)
            out[:, place] = out[:, place] + products[u]
        return nothing

    lax.fori_loop(0, (count + UNROLL - 1) >> UNROLL_BITS, one, 0)
    acc = out[:, :tile]
    for n in range(1, out.shape[1] // tile):
        acc = acc + out[:, n * tile : (n + 1) * tile]
    return acc


def reach_body(up_codes, down_codes, weighted, tiles, to_up, to_down, sums, first, second, work):
    tile = tiles.shape[1]
    acc = run_items(up_codes, 0, weighted, tiles, first, work)
    start = down_codes.shape[1] - second.shape[1] // tile
    to_up[...] = first[...].astype(to_up.dtype)
    acc = acc + run_items(down_codes, start, weighted, tiles, second, work)
    to_down[...] = second[...].astype(to_down.dtype)
    sums[...] = jnp.broadcast_to(row_of(acc), sums.shape)


def local_body(codes, weighted, tiles, reach_sums, totals, peers, raw, sums, work):
    acc = run_items(codes, 0, weighted, tiles, raw, work)
    reached = reach_sums[0:1] + row_of(acc)
    rows = lax.broadcasted_iota(jnp.int32, sums.shape, 0)
    sums[...] = jnp.where(rows == 2, reached, jnp.where(rows == 3, peers[0:1], totals[...]))


def finish_body(raw, from_down, from_up, target, totals, out_hbm, staged, sems):
    columns, cells = raw.shape
    edge = from_down.shape[1]
    piece = edge // 2
    pieces = cells // piece
    correction = (totals[0:1] - totals[2:3]) / totals[1:2]
    spread = jnp.broadcast_to(correction, (128, columns)).T
    spread = jnp.concatenate([spread] * (piece // 128), axis=1)
    copies = []
    for n in range(pieces):
        at = pl.ds(n * piece, piece)
        value = raw[:, at]
        if n * piece < edge:
            value = value + from_down[:, at].astype(jnp.float32)
        if (n + 1) * piece > cells - edge:
            begin = n * piece - (cells - edge)
            value = value + from_up[:, pl.ds(begin, piece)].astype(jnp.float32)
        staged[:, at] = value / target[:, at] + spread
        copies.append(pltpu.make_async_copy(staged.at[:, at], out_hbm.at[:, at], sems.at[n]))
        copies[n].start()
    for copy in copies:
        copy.wait()


def total_over(values, axis):
    size = lax.axis_size(axis)
    if size & (size - 1):
        return lax.psum(values, axis)
    step = 1
    while step < size:
        values = values + lax.ppermute(values, axis, [(i, i ^ step) for i in range(size)])
        step *= 2
    return values


def regrid(
    surface_fields, land_mask, source_area, target_area, weight_tiles, tile_of, block_of, live_slots
):
    members, fields, snapshots, cells = surface_fields.shape
    columns = members * fields * snapshots
    tile_count, tile, _ = weight_tiles.shape
    tgt_count, slots = tile_of.shape
    own_blocks = cells // tile
    stride = own_blocks // tgt_count
    edge = -(-HALO_BLK // stride)
    size = lax.axis_size("band")
    up = [(i, (i + 1) % size) for i in range(size)]
    down = [(j, i) for i, j in up]
    f32 = jnp.float32
    blank = tile_count << PLACE_BITS
    work_size = slots // CHUNK
    listing = jax.ShapeDtypeStruct((slots + 8, tgt_count), jnp.int32)
    in_hbm = lambda x: pltpu.with_memory_space_constraint(x, pltpu.HBM)
    codes, low, high = pl.pallas_call(
        functools.partial(edge_body, own_blocks, blank),
        out_shape=(listing,) * 3,
        in_specs=[ANY] * 3,
        out_specs=(VMEM,) * 3,
        scratch_shapes=[
            pltpu.VMEM((slots, tgt_count), jnp.int32),
            pltpu.VMEM((slots, tgt_count), jnp.int32),
            pltpu.VMEM((1, tgt_count), jnp.int32),
            pltpu.SemaphoreType.DMA((3,)),
        ],
        compiler_params=params(4),
        name="edges",
    )(in_hbm(tile_of.T), in_hbm(block_of.T), in_hbm(live_slots.reshape(1, tgt_count)))
    up_codes = lax.ppermute(low, "band", down)
    down_codes = lax.ppermute(high, "band", up)

    weighted, totals, tiles = pl.pallas_call(
        weigh_body,
        out_shape=(
            jax.ShapeDtypeStruct((columns, cells), jnp.bfloat16),
            jax.ShapeDtypeStruct((8, columns), f32),
            jax.ShapeDtypeStruct((tile_count + 1, tile, tile), jnp.bfloat16),
        ),
        in_specs=[ANY] * 5,
        out_specs=(VMEM,) * 3,
        scratch_shapes=[
            pltpu.VMEM((columns, cells), jnp.bfloat16),
            pltpu.VMEM((1, cells), jnp.int32),
            pltpu.VMEM((1, cells), f32),
            pltpu.VMEM((1, tgt_count * tile), f32),
            pltpu.SemaphoreType.DMA((PIECES + 4,)),
        ],
        compiler_params=params(16),
        name="weigh",
    )(
        in_hbm(surface_fields.reshape(columns, cells)),
        in_hbm(land_mask.reshape(1, cells)),
        in_hbm(source_area.reshape(1, cells)),
        in_hbm(target_area.reshape(1, tgt_count * tile)),
        in_hbm(weight_tiles),
    )
    peers = total_over(totals, "mem")

    to_up, to_down, reach_sums = pl.pallas_call(
        reach_body,
        out_shape=(
            jax.ShapeDtypeStruct((columns, edge * tile), jnp.bfloat16),
            jax.ShapeDtypeStruct((columns, edge * tile), jnp.bfloat16),
            jax.ShapeDtypeStruct((8, columns), f32),
        ),
        in_specs=[SMEM, SMEM, VMEM, VMEM],
        out_specs=(VMEM, VMEM, VMEM),
        scratch_shapes=[pltpu.VMEM((columns, edge * tile), f32)] * 2
        + [pltpu.SMEM((edge * work_size + 8,), jnp.int32)],
        compiler_params=params(8),
        name="reach",
    )(up_codes, down_codes, weighted, tiles)
    from_down = lax.ppermute(to_up, "band", up)
    from_up = lax.ppermute(to_down, "band", down)

    raw, sums = pl.pallas_call(
        local_body,
        out_shape=(
            jax.ShapeDtypeStruct((columns, tgt_count * tile), f32),
            jax.ShapeDtypeStruct((8, columns), f32),
        ),
        in_specs=[SMEM, VMEM, VMEM, VMEM, VMEM, VMEM],
        out_specs=(VMEM, VMEM),
        scratch_shapes=[pltpu.SMEM((tgt_count * work_size + 8,), jnp.int32)],
        compiler_params=params(8),
        name="local",
    )(codes, weighted, tiles, reach_sums, totals, peers)
    totals = total_over(sums, "band")

    piece_count = 2 * tgt_count // edge
    regridded = pl.pallas_call(
        finish_body,
        out_shape=jax.ShapeDtypeStruct((columns, tgt_count * tile), f32),
        in_specs=[VMEM] * 5,
        out_specs=ANY,
        scratch_shapes=[
            pltpu.VMEM((columns, tgt_count * tile), f32),
            pltpu.SemaphoreType.DMA((piece_count,)),
        ],
        compiler_params=params(16),
        name="finish",
    )(raw, from_down, from_up, target_area.reshape(1, tgt_count * tile), totals)

    conserved = (totals[0] / totals[1]).reshape(members, fields, snapshots)
    ensemble = jnp.sum((totals[3] / totals[1]).reshape(members, fields, snapshots), axis=0) / MEMBERS
    return regridded.reshape(members, fields, snapshots, tgt_count * tile), conserved, ensemble


def solution(mesh):
    placed = (
        P(("grp", "mem"), "fld", None, "band"),
        P("band"),
        P("band"),
        P("band"),
        P(),
        P("band", None),
        P("band", None),
        P("band"),
    )
    return jax.shard_map(
        regrid,
        mesh=mesh,
        in_specs=placed,
        out_specs=(
            P(("grp", "mem"), "fld", None, "band"),
            P(("grp", "mem"), "fld", None),
            P(("grp", "fld"), None),
        ),
        check_vma=False,
    )
```

```python
import functools

import jax
import jax.numpy as jnp
from jax import lax
from jax.experimental import pallas as pl
from jax.experimental.pallas import tpu as pltpu
from jax.sharding import PartitionSpec as P


MEMBERS = 8
HALO_BLK = 32
CHUNK = 4
CHUNK_BITS = 2
UNROLL = 8
UNROLL_BITS = 3
PIECES = 8
PLACE_BITS = 16

VMEM = pl.BlockSpec(memory_space=pltpu.VMEM)
SMEM = pl.BlockSpec(memory_space=pltpu.SMEM)
ANY = pl.BlockSpec(memory_space=pl.ANY)


def params(mib):
    return pltpu.CompilerParams(vmem_limit_bytes=mib * 1024 * 1024)


def row_of(acc):
    return jnp.sum(acc.T, axis=0, keepdims=True)


def packed(mask, code, blank):
    slots, targets = code.shape
    ones = jnp.where(mask, 1.0, 0.0)
    above = lax.broadcasted_iota(jnp.int32, (slots, slots), 0)
    below = lax.broadcasted_iota(jnp.int32, (slots, slots), 1)
    before = jnp.where(below < above, 1.0, 0.0).astype(jnp.bfloat16)
    rank = jnp.dot(before, ones.astype(jnp.bfloat16), preferred_element_type=jnp.float32)
    rank = jnp.where(mask, rank, -1.0).astype(jnp.int32)
    extra = (code - blank).astype(jnp.float32)
    rows = [
        jnp.sum(jnp.where(rank == p, extra, 0.0), axis=0, keepdims=True) for p in range(slots)
    ]
    body = jnp.concatenate(rows, axis=0).astype(jnp.int32) + blank
    counts = jnp.sum(ones, axis=0, keepdims=True).astype(jnp.int32)
    row = lax.broadcasted_iota(jnp.int32, (8, targets), 0)
    return jnp.concatenate([body, jnp.where(row == 0, counts, blank)], axis=0)


def edge_body(own_blocks, blank, tile_hbm, block_hbm, live_hbm, own, low, high, tiles, blocks, live, sems):
    copies = [
        pltpu.make_async_copy(source, place, sems.at[n])
        for n, (source, place) in enumerate(((tile_hbm, tiles), (block_hbm, blocks), (live_hbm, live)))
    ]
    for copy in copies:
        copy.start()
    for copy in copies:
        copy.wait()
    band = lax.axis_index("band")
    slot = lax.broadcasted_iota(jnp.int32, tiles.shape, 0)
    alive = slot < live[...]
    block = blocks[...] - HALO_BLK
    code = (tiles[...] << PLACE_BITS) + block
    below = jnp.where(band > 0, 0, -HALO_BLK)
    above = jnp.where(band < lax.axis_size("band") - 1, own_blocks, own_blocks + HALO_BLK)
    low[...] = packed(alive & (block < below), code + own_blocks, blank)
    high[...] = packed(alive & (block >= above), code - own_blocks, blank)
    own[...] = packed(alive & (block >= 0) & (block < own_blocks), code, blank)


def cell_weights(codes, tiles, tile_count, own_blocks):
    slots, targets = codes.shape[0] - 8, codes.shape[1]
    tile = tiles.shape[1]
    last = (((1,), (1,)), ((), ()))
    line = jnp.concatenate([codes[k : k + 1, :] for k in range(slots)], axis=1)
    length = slots * targets
    blocks = lax.broadcasted_iota(jnp.int32, (own_blocks, length), 0)
    kinds = lax.broadcasted_iota(jnp.int32, (tile_count, length), 0)
    reads = jnp.where(blocks == (line & ((1 << PLACE_BITS) - 1)), 1.0, 0.0).astype(jnp.bfloat16)
    uses = jnp.where(kinds == (line >> PLACE_BITS), 1.0, 0.0).astype(jnp.bfloat16)
    counts = lax.dot_general(reads, uses, last, preferred_element_type=jnp.float32)
    flat = tiles[pl.ds(0, tile_count)].reshape(tile_count * tile, tiles.shape[2])
    ones = jnp.ones((8, tiles.shape[2]), jnp.bfloat16)
    sums = lax.dot_general(ones, flat, last, preferred_element_type=jnp.float32)
    sums = jnp.concatenate([sums[0:1, k * tile : (k + 1) * tile] for k in range(tile_count)], axis=0)
    return jnp.dot(
        counts, sums, precision=lax.Precision.HIGHEST, preferred_element_type=jnp.float32
    )


def weigh_body(
    fields_hbm, mask_hbm, area_hbm, target_hbm, tiles_hbm, codes,
    weighted, totals, tiles, fields, mask, source, target, spread, sems,
):
    columns, cells = weighted.shape
    tile_count, tile, lanes = tiles_hbm.shape
    step = 4 * tile
    piece = cells // PIECES
    small = [
        pltpu.make_async_copy(mask_hbm, mask, sems.at[PIECES]),
        pltpu.make_async_copy(area_hbm, source, sems.at[PIECES + 1]),
        pltpu.make_async_copy(target_hbm, target, sems.at[PIECES + 2]),
        pltpu.make_async_copy(tiles_hbm, tiles.at[pl.ds(0, tile_count)], sems.at[PIECES + 3]),
    ]
    copies = [
        pltpu.make_async_copy(
            fields_hbm.at[:, pl.ds(n * piece, piece)],
            fields.at[:, pl.ds(n * piece, piece)],
            sems.at[n],
        )
        for n in range(PIECES)
    ]
    for copy in small + copies:
        copy.start()
    tiles[tile_count] = jnp.zeros((tile, lanes), tiles.dtype)
    for copy in small:
        copy.wait()
    spread[...] = cell_weights(codes, tiles, tile_count, cells // tile)
    area = jnp.sum(target[...], axis=1, keepdims=True)
    accs = (jnp.zeros((columns, tile), jnp.float32),) * 2
    for n in range(PIECES):
        copies[n].wait()

        def one(k, accs):
            acc, reached = accs
            at = pl.ds(pl.multiple_of(n * piece + k * step, step), step)
            factor = source[:, at] * mask[:, at].astype(jnp.float32)
            value = (factor * fields[:, at].astype(jnp.float32)).astype(jnp.bfloat16)
            weighted[:, at] = value
            wide = value.astype(jnp.float32)
            for q in range(4):
                part = wide[:, q * tile : (q + 1) * tile]
                acc = acc + part
                reached = reached + part * spread[pl.ds(n * (piece // tile) + k * 4 + q, 1), :]
            return acc, reached

        accs = lax.fori_loop(0, piece // step, one, accs)
    own = row_of(accs[0])
    reached = row_of(accs[1])
    rows = lax.broadcasted_iota(jnp.int32, (8, columns), 0)
    rest = jnp.where(rows == 1, area, jnp.where(rows == 2, reached, 0.0))
    totals[...] = jnp.where(rows == 0, own, rest)


def run_items(codes, weighted, tiles, out, work):
    tile = tiles.shape[1]
    slots = codes.shape[0] - 8
    chunks = slots // CHUNK
    out[...] = jnp.zeros(out.shape, out.dtype)

    def one_target(n, items):
        for q in range(chunks):
            work[items + q] = (q << PLACE_BITS) + n
        return items + ((codes[slots, n] + CHUNK - 1) >> CHUNK_BITS)

    count = lax.fori_loop(0, out.shape[1] // tile, one_target, 0)
    for q in range(UNROLL):
        work[count + q] = (slots + 4) // CHUNK << PLACE_BITS

    def one(step, nothing):
        products = []
        for u in range(UNROLL):
            item = work[step * UNROLL + u]
            row = (item >> PLACE_BITS) * CHUNK
            column = item & ((1 << PLACE_BITS) - 1)
            left, right = [], []
            for q in range(CHUNK):
                code = codes[row + q, column]
                block = code & ((1 << PLACE_BITS) - 1)
                left.append(weighted[:, pl.ds(pl.multiple_of(block * tile, tile), tile)])
                right.append(tiles[code >> PLACE_BITS])
            products.append(
                jnp.dot(
                    jnp.concatenate(left, axis=1),
                    jnp.concatenate(right, axis=0),
                    preferred_element_type=jnp.float32,
                )
            )
        for u in range(UNROLL):
            target = work[step * UNROLL + u] & ((1 << PLACE_BITS) - 1)
            place = pl.ds(pl.multiple_of(target * tile, tile), tile)
            out[:, place] = out[:, place] + products[u]
        return nothing

    lax.fori_loop(0, (count + UNROLL - 1) >> UNROLL_BITS, one, 0)


def reach_body(codes, weighted, tiles, totals, to_up, to_down, sums, out, work):
    tile = tiles.shape[1]
    run_items(codes, weighted, tiles, out, work)
    half = to_up.shape[1]
    to_up[...] = out[:, :half].astype(to_up.dtype)
    to_down[...] = out[:, half:].astype(to_down.dtype)
    acc = out[:, :tile]
    for n in range(1, out.shape[1] // tile):
        acc = acc + out[:, n * tile : (n + 1) * tile]
    rows = lax.broadcasted_iota(jnp.int32, sums.shape, 0)
    sums[...] = totals[...] + jnp.where(rows == 2, row_of(acc), 0.0)


def local_body(codes, weighted, tiles, raw, work):
    run_items(codes, weighted, tiles, raw, work)


def finish_body(
    raw, from_down, from_up, target, totals, out_hbm, conserved, ensemble, staged, sems
):
    columns, cells = raw.shape
    edge = from_down.shape[1]
    piece = edge // 2
    pieces = cells // piece
    correction = (totals[0:1] - totals[2:3]) / totals[1:2]
    spread = jnp.broadcast_to(correction, (128, columns)).T
    spread = jnp.concatenate([spread] * (piece // 128), axis=1)
    copies = []
    for n in range(pieces):
        at = pl.ds(n * piece, piece)
        value = raw[:, at]
        if n * piece < edge:
            value = value + from_down[:, at].astype(jnp.float32)
        if (n + 1) * piece > cells - edge:
            begin = n * piece - (cells - edge)
            value = value + from_up[:, pl.ds(begin, piece)].astype(jnp.float32)
        staged[:, at] = value / target[:, at] + spread
        copies.append(pltpu.make_async_copy(staged.at[:, at], out_hbm.at[:, at], sems.at[n]))
        copies[n].start()
    members, fields, snapshots = conserved.shape
    own = totals[0:1] / totals[1:2]
    every = totals[3:4] / totals[1:2]
    for f in range(fields):
        mean = jnp.zeros((1, snapshots), jnp.float32)
        for m in range(members):
            begin = (m * fields + f) * snapshots
            conserved[m, f : f + 1, :] = own[:, begin : begin + snapshots]
            mean = mean + every[:, begin : begin + snapshots]
        ensemble[f : f + 1, :] = mean / MEMBERS
    for copy in copies:
        copy.wait()


def total_over(values, axis):
    size = lax.axis_size(axis)
    if size & (size - 1):
        return lax.psum(values, axis)
    if size == 4:
        terms = [values]
        for step in range(1, size):
            terms.append(lax.ppermute(values, axis, [(i, i ^ step) for i in range(size)]))
        return (terms[0] + terms[1]) + (terms[2] + terms[3])
    step = 1
    while step < size:
        values = values + lax.ppermute(values, axis, [(i, i ^ step) for i in range(size)])
        step *= 2
    return values


def regrid(
    surface_fields, land_mask, source_area, target_area, weight_tiles, tile_of, block_of, live_slots
):
    members, fields, snapshots, cells = surface_fields.shape
    columns = members * fields * snapshots
    tile_count, tile, _ = weight_tiles.shape
    tgt_count, slots = tile_of.shape
    own_blocks = cells // tile
    stride = own_blocks // tgt_count
    edge = -(-HALO_BLK // stride)
    size = lax.axis_size("band")
    up = [(i, (i + 1) % size) for i in range(size)]
    down = [(j, i) for i, j in up]
    f32 = jnp.float32
    blank = tile_count << PLACE_BITS
    work_size = slots // CHUNK
    listing = jax.ShapeDtypeStruct((slots + 8, tgt_count), jnp.int32)
    in_hbm = lambda x: pltpu.with_memory_space_constraint(x, pltpu.HBM)
    codes, low, high = pl.pallas_call(
        functools.partial(edge_body, own_blocks, blank),
        out_shape=(listing,) * 3,
        in_specs=[ANY] * 3,
        out_specs=(VMEM,) * 3,
        scratch_shapes=[
            pltpu.VMEM((slots, tgt_count), jnp.int32),
            pltpu.VMEM((slots, tgt_count), jnp.int32),
            pltpu.VMEM((1, tgt_count), jnp.int32),
            pltpu.SemaphoreType.DMA((3,)),
        ],
        compiler_params=params(4),
        name="edges",
    )(in_hbm(tile_of.T), in_hbm(block_of.T), in_hbm(live_slots.reshape(1, tgt_count)))
    up_codes = lax.ppermute(low, "band", down)
    down_codes = lax.ppermute(high, "band", up)

    weighted, totals, tiles = pl.pallas_call(
        weigh_body,
        out_shape=(
            jax.ShapeDtypeStruct((columns, cells), jnp.bfloat16),
            jax.ShapeDtypeStruct((8, columns), f32),
            jax.ShapeDtypeStruct((tile_count + 1, tile, tile), jnp.bfloat16),
        ),
        in_specs=[ANY] * 5 + [VMEM],
        out_specs=(VMEM,) * 3,
        scratch_shapes=[
            pltpu.VMEM((columns, cells), jnp.bfloat16),
            pltpu.VMEM((1, cells), jnp.int32),
            pltpu.VMEM((1, cells), f32),
            pltpu.VMEM((1, tgt_count * tile), f32),
            pltpu.VMEM((own_blocks, tile), f32),
            pltpu.SemaphoreType.DMA((PIECES + 4,)),
        ],
        compiler_params=params(16),
        name="weigh",
    )(
        in_hbm(surface_fields.reshape(columns, cells)),
        in_hbm(land_mask.reshape(1, cells)),
        in_hbm(source_area.reshape(1, cells)),
        in_hbm(target_area.reshape(1, tgt_count * tile)),
        in_hbm(weight_tiles),
        codes,
    )
    peers = total_over(totals, "mem")

    reach_codes = jnp.concatenate([up_codes[:, :edge], down_codes[:, tgt_count - edge :]], axis=1)
    to_up, to_down, sums = pl.pallas_call(
        reach_body,
        out_shape=(
            jax.ShapeDtypeStruct((columns, edge * tile), jnp.bfloat16),
            jax.ShapeDtypeStruct((columns, edge * tile), jnp.bfloat16),
            jax.ShapeDtypeStruct((8, columns), f32),
        ),
        in_specs=[SMEM, VMEM, VMEM, VMEM],
        out_specs=(VMEM,) * 3,
        scratch_shapes=[
            pltpu.VMEM((columns, 2 * edge * tile), f32),
            pltpu.SMEM((2 * edge * work_size + 16,), jnp.int32),
        ],
        compiler_params=params(8),
        name="reach",
    )(reach_codes, weighted, tiles, totals)
    from_down = lax.ppermute(to_up, "band", up)
    from_up = lax.ppermute(to_down, "band", down)
    rows = lax.broadcasted_iota(jnp.int32, sums.shape, 0)
    totals = total_over(jnp.where(rows == 3, peers[0:1], sums), "band")

    raw = pl.pallas_call(
        local_body,
        out_shape=jax.ShapeDtypeStruct((columns, tgt_count * tile), f32),
        in_specs=[SMEM, VMEM, VMEM],
        out_specs=VMEM,
        scratch_shapes=[pltpu.SMEM((tgt_count * work_size + 16,), jnp.int32)],
        compiler_params=params(8),
        name="local",
    )(codes, weighted, tiles)

    piece_count = 2 * tgt_count // edge
    regridded, conserved, ensemble = pl.pallas_call(
        finish_body,
        out_shape=(
            jax.ShapeDtypeStruct((columns, tgt_count * tile), f32),
            jax.ShapeDtypeStruct((members, fields, snapshots), f32),
            jax.ShapeDtypeStruct((fields, snapshots), f32),
        ),
        in_specs=[VMEM] * 5,
        out_specs=(ANY, VMEM, VMEM),
        scratch_shapes=[
            pltpu.VMEM((columns, tgt_count * tile), f32),
            pltpu.SemaphoreType.DMA((piece_count,)),
        ],
        compiler_params=params(16),
        name="finish",
    )(raw, from_down, from_up, target_area.reshape(1, tgt_count * tile), totals)

    return regridded.reshape(members, fields, snapshots, tgt_count * tile), conserved, ensemble


def solution(mesh):
    placed = (
        P(("grp", "mem"), "fld", None, "band"),
        P("band"),
        P("band"),
        P("band"),
        P(),
        P("band", None),
        P("band", None),
        P("band"),
    )
    return jax.shard_map(
        regrid,
        mesh=mesh,
        in_specs=placed,
        out_specs=(
            P(("grp", "mem"), "fld", None, "band"),
            P(("grp", "mem"), "fld", None),
            P(("grp", "fld"), None),
        ),
        check_vma=False,
    )
```

```python
import functools

import jax
import jax.numpy as jnp
from jax import lax
from jax.experimental import pallas as pl
from jax.experimental.pallas import tpu as pltpu
from jax.sharding import PartitionSpec as P


MEMBERS = 8
HALO_BLK = 32
CHUNK = 4
CHUNK_BITS = 2
REACH_BITS = 3
LOCAL_BITS = 4
PIECES = 8
PLACE_BITS = 16

VMEM = pl.BlockSpec(memory_space=pltpu.VMEM)
SMEM = pl.BlockSpec(memory_space=pltpu.SMEM)
ANY = pl.BlockSpec(memory_space=pl.ANY)


def params(mib):
    return pltpu.CompilerParams(vmem_limit_bytes=mib * 1024 * 1024)


def row_of(acc):
    return jnp.sum(acc.T, axis=0, keepdims=True)


def packed(mask, code, blank):
    slots, targets = code.shape
    ones = jnp.where(mask, 1.0, 0.0)
    above = lax.broadcasted_iota(jnp.int32, (slots, slots), 0)
    below = lax.broadcasted_iota(jnp.int32, (slots, slots), 1)
    before = jnp.where(below < above, 1.0, 0.0).astype(jnp.bfloat16)
    rank = jnp.dot(before, ones.astype(jnp.bfloat16), preferred_element_type=jnp.float32)
    rank = jnp.where(mask, rank, -1.0).astype(jnp.int32)
    extra = (code - blank).astype(jnp.float32)
    rows = [
        jnp.sum(jnp.where(rank == p, extra, 0.0), axis=0, keepdims=True) for p in range(slots)
    ]
    body = jnp.concatenate(rows, axis=0).astype(jnp.int32) + blank
    counts = jnp.sum(ones, axis=0, keepdims=True).astype(jnp.int32)
    row = lax.broadcasted_iota(jnp.int32, (8, targets), 0)
    return jnp.concatenate([body, jnp.where(row == 0, counts, blank)], axis=0)


def edge_body(own_blocks, blank, tile_hbm, block_hbm, live_hbm, own, low, high, tiles, blocks, live, sems):
    copies = [
        pltpu.make_async_copy(source, place, sems.at[n])
        for n, (source, place) in enumerate(((tile_hbm, tiles), (block_hbm, blocks), (live_hbm, live)))
    ]
    for copy in copies:
        copy.start()
    for copy in copies:
        copy.wait()
    band = lax.axis_index("band")
    slot = lax.broadcasted_iota(jnp.int32, tiles.shape, 0)
    alive = slot < live[...]
    block = blocks[...] - HALO_BLK
    code = (tiles[...] << PLACE_BITS) + block
    below = jnp.where(band > 0, 0, -HALO_BLK)
    above = jnp.where(band < lax.axis_size("band") - 1, own_blocks, own_blocks + HALO_BLK)
    low[...] = packed(alive & (block < below), code + own_blocks, blank)
    high[...] = packed(alive & (block >= above), code - own_blocks, blank)
    own[...] = packed(alive & (block >= 0) & (block < own_blocks), code, blank)


def cell_weights(codes, tiles, tile_count, own_blocks):
    slots, targets = codes.shape[0] - 8, codes.shape[1]
    tile = tiles.shape[1]
    last = (((1,), (1,)), ((), ()))
    line = jnp.concatenate([codes[k : k + 1, :] for k in range(slots)], axis=1)
    length = slots * targets
    blocks = lax.broadcasted_iota(jnp.int32, (own_blocks, length), 0)
    kinds = lax.broadcasted_iota(jnp.int32, (tile_count, length), 0)
    reads = jnp.where(blocks == (line & ((1 << PLACE_BITS) - 1)), 1.0, 0.0).astype(jnp.bfloat16)
    uses = jnp.where(kinds == (line >> PLACE_BITS), 1.0, 0.0).astype(jnp.bfloat16)
    counts = lax.dot_general(reads, uses, last, preferred_element_type=jnp.float32)
    flat = tiles[pl.ds(0, tile_count)].reshape(tile_count * tile, tiles.shape[2])
    ones = jnp.ones((8, tiles.shape[2]), jnp.bfloat16)
    sums = lax.dot_general(ones, flat, last, preferred_element_type=jnp.float32)
    sums = jnp.concatenate([sums[0:1, k * tile : (k + 1) * tile] for k in range(tile_count)], axis=0)
    return jnp.dot(
        counts, sums, precision=lax.Precision.HIGHEST, preferred_element_type=jnp.float32
    )


def weigh_body(
    fields_hbm, mask_hbm, area_hbm, target_hbm, tiles_hbm, codes,
    weighted, totals, tiles, fields, mask, source, target, spread, sems,
):
    columns, cells = weighted.shape
    tile_count, tile, lanes = tiles_hbm.shape
    step = 4 * tile
    piece = cells // PIECES
    small = [
        pltpu.make_async_copy(mask_hbm, mask, sems.at[PIECES]),
        pltpu.make_async_copy(area_hbm, source, sems.at[PIECES + 1]),
        pltpu.make_async_copy(target_hbm, target, sems.at[PIECES + 2]),
        pltpu.make_async_copy(tiles_hbm, tiles.at[pl.ds(0, tile_count)], sems.at[PIECES + 3]),
    ]
    copies = [
        pltpu.make_async_copy(
            fields_hbm.at[:, pl.ds(n * piece, piece)],
            fields.at[:, pl.ds(n * piece, piece)],
            sems.at[n],
        )
        for n in range(PIECES)
    ]
    for copy in small + copies:
        copy.start()
    tiles[tile_count] = jnp.zeros((tile, lanes), tiles.dtype)
    for copy in small:
        copy.wait()
    spread[...] = cell_weights(codes, tiles, tile_count, cells // tile)
    area = jnp.sum(target[...], axis=1, keepdims=True)
    accs = (jnp.zeros((columns, tile), jnp.float32),) * 2
    for n in range(PIECES):
        copies[n].wait()

        def one(k, accs):
            acc, reached = accs
            at = pl.ds(pl.multiple_of(n * piece + k * step, step), step)
            factor = source[:, at] * mask[:, at].astype(jnp.float32)
            value = (factor * fields[:, at].astype(jnp.float32)).astype(jnp.bfloat16)
            weighted[:, at] = value
            wide = value.astype(jnp.float32)
            for q in range(4):
                part = wide[:, q * tile : (q + 1) * tile]
                acc = acc + part
                reached = reached + part * spread[pl.ds(n * (piece // tile) + k * 4 + q, 1), :]
            return acc, reached

        accs = lax.fori_loop(0, piece // step, one, accs)
    own = row_of(accs[0])
    reached = row_of(accs[1])
    rows = lax.broadcasted_iota(jnp.int32, (8, columns), 0)
    rest = jnp.where(rows == 1, area, jnp.where(rows == 2, reached, 0.0))
    totals[...] = jnp.where(rows == 0, own, rest)


def run_items(codes, weighted, tiles, out, work, bits):
    tile = tiles.shape[1]
    slots = codes.shape[0] - 8
    chunks = slots // CHUNK
    unroll = 1 << bits
    out[...] = jnp.zeros(out.shape, out.dtype)

    def one_target(n, items):
        for q in range(chunks):
            work[items + q] = (q << PLACE_BITS) + n
        return items + ((codes[slots, n] + CHUNK - 1) >> CHUNK_BITS)

    count = lax.fori_loop(0, out.shape[1] // tile, one_target, 0)
    for q in range(unroll):
        work[count + q] = (slots + 4) // CHUNK << PLACE_BITS

    def one(step, nothing):
        products = []
        for u in range(unroll):
            item = work[step * unroll + u]
            row = (item >> PLACE_BITS) * CHUNK
            column = item & ((1 << PLACE_BITS) - 1)
            left, right = [], []
            for q in range(CHUNK):
                code = codes[row + q, column]
                block = code & ((1 << PLACE_BITS) - 1)
                left.append(weighted[:, pl.ds(pl.multiple_of(block * tile, tile), tile)])
                right.append(tiles[code >> PLACE_BITS])
            products.append(
                jnp.dot(
                    jnp.concatenate(left, axis=1),
                    jnp.concatenate(right, axis=0),
                    preferred_element_type=jnp.float32,
                )
            )
        for u in range(unroll):
            target = work[step * unroll + u] & ((1 << PLACE_BITS) - 1)
            place = pl.ds(pl.multiple_of(target * tile, tile), tile)
            out[:, place] = out[:, place] + products[u]
        return nothing

    lax.fori_loop(0, (count + unroll - 1) >> bits, one, 0)


def reach_body(codes, weighted, tiles, totals, to_up, to_down, sums, out, work):
    tile = tiles.shape[1]
    run_items(codes, weighted, tiles, out, work, REACH_BITS)
    half = to_up.shape[1]
    to_up[...] = out[:, :half].astype(to_up.dtype)
    to_down[...] = out[:, half:].astype(to_down.dtype)
    acc = out[:, :tile]
    for n in range(1, out.shape[1] // tile):
        acc = acc + out[:, n * tile : (n + 1) * tile]
    rows = lax.broadcasted_iota(jnp.int32, sums.shape, 0)
    sums[...] = totals[...] + jnp.where(rows == 2, row_of(acc), 0.0)


def local_body(codes, weighted, tiles, raw, work):
    run_items(codes, weighted, tiles, raw, work, LOCAL_BITS)


def finish_body(
    raw, from_down, from_up, target, totals, out_hbm, conserved_hbm, ensemble_hbm,
    staged, conserved, ensemble, sems,
):
    columns, cells = raw.shape
    edge = from_down.shape[1]
    piece = edge // 2
    pieces = cells // piece
    correction = (totals[0:1] - totals[2:3]) / totals[1:2]
    spread = jnp.broadcast_to(correction, (128, columns)).T
    spread = jnp.concatenate([spread] * (piece // 128), axis=1)
    members, fields, snapshots = conserved.shape
    own = totals[0:1] / totals[1:2]
    every = totals[3:4] / totals[1:2]
    for f in range(fields):
        mean = jnp.zeros((1, snapshots), jnp.float32)
        for m in range(members):
            begin = (m * fields + f) * snapshots
            conserved[m, f : f + 1, :] = own[:, begin : begin + snapshots]
            mean = mean + every[:, begin : begin + snapshots]
        ensemble[f : f + 1, :] = mean / MEMBERS
    copies = [
        pltpu.make_async_copy(conserved, conserved_hbm, sems.at[pieces]),
        pltpu.make_async_copy(ensemble, ensemble_hbm, sems.at[pieces + 1]),
    ]
    for copy in copies:
        copy.start()
    for n in range(pieces):
        at = pl.ds(n * piece, piece)
        value = raw[:, at]
        if n * piece < edge:
            value = value + from_down[:, at].astype(jnp.float32)
        if (n + 1) * piece > cells - edge:
            begin = n * piece - (cells - edge)
            value = value + from_up[:, pl.ds(begin, piece)].astype(jnp.float32)
        staged[:, at] = value / target[:, at] + spread
        copies.append(pltpu.make_async_copy(staged.at[:, at], out_hbm.at[:, at], sems.at[n]))
        copies[-1].start()
    for copy in copies:
        copy.wait()


def total_over(values, axis):
    size = lax.axis_size(axis)
    if size & (size - 1):
        return lax.psum(values, axis)
    if size == 4:
        terms = [values]
        for step in range(1, size):
            terms.append(lax.ppermute(values, axis, [(i, i ^ step) for i in range(size)]))
        return (terms[0] + terms[1]) + (terms[2] + terms[3])
    step = 1
    while step < size:
        values = values + lax.ppermute(values, axis, [(i, i ^ step) for i in range(size)])
        step *= 2
    return values


def regrid(
    surface_fields, land_mask, source_area, target_area, weight_tiles, tile_of, block_of, live_slots
):
    members, fields, snapshots, cells = surface_fields.shape
    columns = members * fields * snapshots
    tile_count, tile, _ = weight_tiles.shape
    tgt_count, slots = tile_of.shape
    own_blocks = cells // tile
    stride = own_blocks // tgt_count
    edge = -(-HALO_BLK // stride)
    size = lax.axis_size("band")
    up = [(i, (i + 1) % size) for i in range(size)]
    down = [(j, i) for i, j in up]
    f32 = jnp.float32
    blank = tile_count << PLACE_BITS
    work_size = slots // CHUNK
    listing = jax.ShapeDtypeStruct((slots + 8, tgt_count), jnp.int32)
    in_hbm = lambda x: pltpu.with_memory_space_constraint(x, pltpu.HBM)
    codes, low, high = pl.pallas_call(
        functools.partial(edge_body, own_blocks, blank),
        out_shape=(listing,) * 3,
        in_specs=[ANY] * 3,
        out_specs=(VMEM,) * 3,
        scratch_shapes=[
            pltpu.VMEM((slots, tgt_count), jnp.int32),
            pltpu.VMEM((slots, tgt_count), jnp.int32),
            pltpu.VMEM((1, tgt_count), jnp.int32),
            pltpu.SemaphoreType.DMA((3,)),
        ],
        compiler_params=params(4),
        name="edges",
    )(in_hbm(tile_of.T), in_hbm(block_of.T), in_hbm(live_slots.reshape(1, tgt_count)))
    up_codes = lax.ppermute(low, "band", down)
    down_codes = lax.ppermute(high, "band", up)

    weighted, totals, tiles = pl.pallas_call(
        weigh_body,
        out_shape=(
            jax.ShapeDtypeStruct((columns, cells), jnp.bfloat16),
            jax.ShapeDtypeStruct((8, columns), f32),
            jax.ShapeDtypeStruct((tile_count + 1, tile, tile), jnp.bfloat16),
        ),
        in_specs=[ANY] * 5 + [VMEM],
        out_specs=(VMEM,) * 3,
        scratch_shapes=[
            pltpu.VMEM((columns, cells), jnp.bfloat16),
            pltpu.VMEM((1, cells), jnp.int32),
            pltpu.VMEM((1, cells), f32),
            pltpu.VMEM((1, tgt_count * tile), f32),
            pltpu.VMEM((own_blocks, tile), f32),
            pltpu.SemaphoreType.DMA((PIECES + 4,)),
        ],
        compiler_params=params(16),
        name="weigh",
    )(
        in_hbm(surface_fields.reshape(columns, cells)),
        in_hbm(land_mask.reshape(1, cells)),
        in_hbm(source_area.reshape(1, cells)),
        in_hbm(target_area.reshape(1, tgt_count * tile)),
        in_hbm(weight_tiles),
        codes,
    )
    peers = total_over(totals, "mem")

    reach_codes = jnp.concatenate([up_codes[:, :edge], down_codes[:, tgt_count - edge :]], axis=1)
    to_up, to_down, sums = pl.pallas_call(
        reach_body,
        out_shape=(
            jax.ShapeDtypeStruct((columns, edge * tile), jnp.bfloat16),
            jax.ShapeDtypeStruct((columns, edge * tile), jnp.bfloat16),
            jax.ShapeDtypeStruct((8, columns), f32),
        ),
        in_specs=[SMEM, VMEM, VMEM, VMEM],
        out_specs=(VMEM,) * 3,
        scratch_shapes=[
            pltpu.VMEM((columns, 2 * edge * tile), f32),
            pltpu.SMEM((2 * edge * work_size + 16,), jnp.int32),
        ],
        compiler_params=params(8),
        name="reach",
    )(reach_codes, weighted, tiles, totals)
    from_down = lax.ppermute(to_up, "band", up)
    from_up = lax.ppermute(to_down, "band", down)
    rows = lax.broadcasted_iota(jnp.int32, sums.shape, 0)
    totals = total_over(jnp.where(rows == 3, peers[0:1], sums), "band")

    raw = pl.pallas_call(
        local_body,
        out_shape=jax.ShapeDtypeStruct((columns, tgt_count * tile), f32),
        in_specs=[SMEM, VMEM, VMEM],
        out_specs=VMEM,
        scratch_shapes=[pltpu.SMEM((tgt_count * work_size + 16,), jnp.int32)],
        compiler_params=params(8),
        name="local",
    )(codes, weighted, tiles)

    piece_count = 2 * tgt_count // edge
    regridded, conserved, ensemble = pl.pallas_call(
        finish_body,
        out_shape=(
            jax.ShapeDtypeStruct((columns, tgt_count * tile), f32),
            jax.ShapeDtypeStruct((members, fields, snapshots), f32),
            jax.ShapeDtypeStruct((fields, snapshots), f32),
        ),
        in_specs=[VMEM] * 5,
        out_specs=(ANY,) * 3,
        scratch_shapes=[
            pltpu.VMEM((columns, tgt_count * tile), f32),
            pltpu.VMEM((members, fields, snapshots), f32),
            pltpu.VMEM((fields, snapshots), f32),
            pltpu.SemaphoreType.DMA((piece_count + 2,)),
        ],
        compiler_params=params(16),
        name="finish",
    )(raw, from_down, from_up, target_area.reshape(1, tgt_count * tile), totals)

    return regridded.reshape(members, fields, snapshots, tgt_count * tile), conserved, ensemble


def solution(mesh):
    placed = (
        P(("grp", "mem"), "fld", None, "band"),
        P("band"),
        P("band"),
        P("band"),
        P(),
        P("band", None),
        P("band", None),
        P("band"),
    )
    return jax.shard_map(
        regrid,
        mesh=mesh,
        in_specs=placed,
        out_specs=(
            P(("grp", "mem"), "fld", None, "band"),
            P(("grp", "mem"), "fld", None),
            P(("grp", "fld"), None),
        ),
        check_vma=False,
    )
```
